32 devices in a mesh: dp: 4 (over z), expert: 2 (over x), shard: 4 (over y, core).
Axes of the slice: x: 2, y: 2, z: 4, core: 2. Of those that a mesh axis runs over, the one named last changes fastest.
Arguments:
- activations: bfloat16 [2, 2, 2048, 256], P(None, 'expert', ('dp', 'shard')), may hold values from -6 to 6
- out_grads: bfloat16 [2, 2, 2048, 14336], P(None, 'expert', ('dp', 'shard')), may hold values from -0.25 to 0.25
- weights: float32 [2, 2, 256, 14336], P(None, 'expert', ('dp', 'shard')), may hold values from -4 to 4
- shadow: float32 [2, 2, 256, 14336], P(None, 'expert', ('dp', 'shard')), may hold values from -4 to 4
- counts: int32 [2, 32, 2], P(None, ('dp', 'expert', 'shard')), may hold values from 1 to 1024, as said below
Outputs:
- new_weights: float32 [2, 2, 256, 14336], P(None, 'expert', ('dp', 'shard'))
- new_shadow: float32 [2, 2, 256, 14336], P(None, 'expert', ('dp', 'shard'))
The draws below stay inside these ranges and needn't reach their ends.
Inputs may be any that keep to these rules, and one draw needn't show every extreme that they name: `counts`: loads differ between the experts of a layer.
All inputs are finite; a program needn't handle non-finite values.
Results may differ from the reference program's by a relative error of at most 0.0003.
Values sent between devices are 32-bit elements; how exact they have to be, the bound alone decides.
A program may use at most 128 MiB of HBM per device.

```python
import jax
import jax.numpy as jnp
from jax import lax

FF = 14336
ROWS = 256
TOK_DEV = 128
LAYERS = 2
EXPERTS = 2
TOKENS = 2048
DEVICES = 32


def draw_activations(key, part):
    base = jax.random.normal(key, (LAYERS, EXPERTS, TOKENS, ROWS), jnp.float32)
    return jnp.clip(base, -6.0, 6.0).astype(jnp.bfloat16)


def draw_out_grads(key, part):
    base = 0.03 * jax.random.normal(key, (LAYERS, EXPERTS, TOKENS, FF), jnp.float32)
    return jnp.clip(base, -0.25, 0.25).astype(jnp.bfloat16)


def draw_counts(key, part):
    ranges = jax.random.randint(jax.random.fold_in(key, 3), (LAYERS, 1, EXPERTS), 1, 9)
    raw = jax.random.randint(key, (LAYERS, DEVICES, EXPERTS), 0, 1 << 20)
    values = 1 + raw % (TOK_DEV * ranges)
    chosen_device = jax.random.randint(jax.random.fold_in(key, 5), (LAYERS, 1, 1), 0, DEVICES)
    chosen_expert = jax.random.randint(jax.random.fold_in(key, 6), (LAYERS, 1, 1), 0, EXPERTS)
    device_ids = jnp.arange(DEVICES, dtype=jnp.int32)[None, :, None]
    expert_ids = jnp.arange(EXPERTS, dtype=jnp.int32)[None, None, :]
    marked = (device_ids == chosen_device) & (expert_ids == chosen_expert)
    values = jnp.where(marked, 8 * TOK_DEV, values)
    return values.astype(jnp.int32)


def levels(key, dims, pieces, low, largest):
    level, own = 1.0, jax.random.fold_in(key, 6)
    for axis_at, parts in pieces:
        steps = jnp.exp(jax.random.uniform(jax.random.fold_in(own, axis_at), (parts,), jnp.float32, low / len(pieces), largest / len(pieces)))
        level = level * jnp.repeat(steps, dims[axis_at] // parts).reshape([-1 if axis == axis_at else 1 for axis in range(len(dims))])
    return level


def normal_values(stream_key, dims, spread, reach, pieces=(), held_as=jnp.bfloat16):
    drawn = spread * jax.random.normal(stream_key, dims, jnp.float32)
    if pieces:
        drawn = drawn * levels(stream_key, dims, pieces, -0.22, 0.18)
    return jnp.clip(drawn, -reach, reach).astype(held_as)


def setup_inputs(seed: int = 0) -> dict:
    streams_of = jax.random.split(jax.random.key(seed), 6)
    return {
        "activations": draw_activations(jax.random.fold_in(streams_of[5], 71), 0),
        "out_grads": draw_out_grads(jax.random.fold_in(streams_of[5], 71), 0),
        "weights": normal_values(streams_of[2], (LAYERS, EXPERTS, ROWS, FF), 0.5, 4.0, ((1, 2), (2, 16)), jnp.float32),
        "shadow": normal_values(streams_of[3], (LAYERS, EXPERTS, ROWS, FF), 0.5, 4.0, ((1, 2), (2, 16)), jnp.float32),
        "counts": draw_counts(jax.random.fold_in(streams_of[5], 71), 0),
    }


step_size = 0.5
clip_level = 1.0

def reference(activations, out_grads, weights, shadow, counts):
    totals = lax.optimization_barrier(jnp.sum(counts, axis=1, dtype=jnp.int32))
    all_weights = []
    all_shadow = []
    for layer_index in range(LAYERS):
        loads = totals[layer_index].astype(jnp.float32)
        mean_load = jnp.mean(loads)

        def update_one(item):
            inputs, cotangent, current, smooth, own_load = item
            summed = jnp.dot(inputs.T, cotangent, preferred_element_type=jnp.float32)
            numel = summed.shape[0] * summed.shape[1]
            root_mean = jnp.sqrt(jnp.sum(summed * summed) / numel)
            factor = step_size * (own_load / mean_load) * clip_level / jnp.maximum(root_mean, clip_level)
            updated = current - factor * summed
            beta = own_load / (own_load + mean_load)
            return (updated, smooth + beta * (updated - smooth))
        updated, smoothed = lax.map(update_one, (activations[layer_index], out_grads[layer_index], weights[layer_index], shadow[layer_index], loads))
        all_weights.append(updated)
        all_shadow.append(smoothed)
    return (jnp.stack(all_weights), jnp.stack(all_shadow))
```

```python
import functools

import jax
import jax.numpy as jnp
from jax import lax
from jax.experimental import pallas as pl
from jax.experimental.pallas import tpu as pltpu
from jax.sharding import PartitionSpec as P

step_size = 0.5
clip_level = 1.0
CORES = 2
SLOTS = 4
LAG = 3
COLS = 256
MESH = pl.DeviceIdType.MESH


def kernel(
    dims, rows_ref, cot_ref, cnt_ref, out_ref, stat_ref,
    merged, from_y, from_z, from_zx, late_y, staged, squares, seen, message, gathered,
    core_send, core_recv, y_send, y_recv, z_send, z_recv, zx_send, zx_recv,
    late_send, late_recv, cnt_send, cnt_recv, all_send, all_recv,
):
    line, experts, shards, layers, per_layer, width, rows, numel = dims
    group = line * shards
    half = line * rows
    chunks = layers * per_layer
    z, e, s = lax.axis_index("dp"), lax.axis_index("expert"), lax.axis_index("shard")
    y, c = s // CORES, s % CORES
    me = z * shards + s
    core_peer = {"shard": y * CORES + (1 - c)}
    y_peer = {"shard": (1 - y) * CORES + c}
    own, other = y * half, (1 - y) * half

    def group_peer(d):
        p = lax.rem(me + d, group)
        return p, {"dp": p // shards, "shard": p % shards}

    def remote(src, dst, send, recv, device):
        return pltpu.make_async_remote_copy(
            src_ref=src, dst_ref=dst, send_sem=send, recv_sem=recv,
            device_id=device, device_id_type=MESH,
        )

    barrier = pltpu.get_barrier_semaphore()
    for d in range(1, group):
        pl.semaphore_signal(barrier, inc=1, device_id=group_peer(d)[1], device_id_type=MESH)
    for d in range(1, experts):
        pl.semaphore_signal(
            barrier, inc=1, device_id={"expert": lax.rem(e + d, experts)}, device_id_type=MESH
        )
    pl.semaphore_wait(barrier, group + experts - 2)

    def count_copy(d, sender):
        return remote(
            cnt_ref, seen.at[sender], cnt_send.at[d], cnt_recv.at[sender],
            {"expert": lax.rem(e + d, experts)},
        )

    for d in range(1, experts):
        count_copy(d, e).start()
    squares[...] = jnp.zeros_like(squares)

    def place(k):
        return k // per_layer, k % per_layer

    def when_chunk(k, body):
        pl.when((k >= 0) & (k < chunks))(lambda: body(k))

    def core_copy(k):
        return remote(
            staged.at[k % SLOTS], merged.at[k], core_send.at[k % SLOTS], core_recv.at[k], core_peer
        )

    def y_copy(k):
        return remote(
            merged.at[k, pl.ds(pl.multiple_of(other, 8), half)], from_y.at[k],
            y_send.at[k], y_recv.at[k], y_peer,
        )

    def late_copy(layer):
        k = layer * per_layer
        return remote(
            merged.at[k, pl.ds(pl.multiple_of(other + z * rows, 8), rows)], late_y.at[layer],
            late_send.at[layer], late_recv.at[layer], y_peer,
        )

    def product(layer, q, core, i):
        at = pl.ds(pl.multiple_of(q * width + i * COLS, 128), COLS)
        return jnp.dot(
            rows_ref[layer, core], cot_ref[layer, :, at], preferred_element_type=jnp.float32
        )

    def stage_partner(k):
        layer, q = place(k)
        pl.when(k >= SLOTS)(lambda: core_copy(k - SLOTS).wait_send())

        def tile(i, _):
            at = pl.ds(pl.multiple_of(i * COLS, 128), COLS)
            staged[k % SLOTS, :, at] = product(layer, q, 1 - c, i)
            return 0

        lax.fori_loop(0, width // COLS, tile, 0)
        core_copy(k).start()

    def merge_core(k):
        layer, q = place(k)
        core_copy(k).wait_recv()

        def tile(i, _):
            at = pl.ds(pl.multiple_of(i * COLS, 128), COLS)
            merged[k, :, at] = merged[k, :, at] + product(layer, q, c, i)
            return 0

        lax.fori_loop(0, width // COLS, tile, 0)
        pl.when(q > 0)(lambda: y_copy(k).start())

    def merge_y(k):
        @pl.when(k % per_layer > 0)
        def _():
            y_copy(k).wait_recv()
            at = pl.ds(pl.multiple_of(own, 8), half)
            merged[k, at, :] = merged[k, at, :] + from_y[k]

    def block(k, base, b):
        return merged.at[k, pl.ds(pl.multiple_of(base + b * rows, 8), rows)]

    def z_copy(k, base, b, slot, device, extra):
        layer = k // per_layer
        if extra:
            return remote(
                block(k, base, b), from_zx.at[layer, slot], zx_send.at[layer, b],
                zx_recv.at[layer, slot], device,
            )
        return remote(
            block(k, base, b), from_z.at[k, slot], z_send.at[k, b], z_recv.at[k, slot], device
        )

    def arrived(k, slot, extra):
        return from_zx[k // per_layer, slot] if extra else from_z[k, slot]

    def add_arrived(k, base, b, slot, extra):
        z_copy(k, base, b, slot, {"dp": z}, extra).wait_recv()
        ref = block(k, base, b)
        ref[...] = ref[...] + arrived(k, slot, extra)

    def to_right(k, base, extra):
        for b in reversed(range(1, line)):
            @pl.when(z < b)
            def _():
                pl.when(z > 0)(lambda: add_arrived(k, base, b, b + 1, extra))
                z_copy(k, base, b, b + 1, {"dp": z + 1}, extra).start()

    def to_left(k, base, extra):
        for b in range(line - 1):
            @pl.when(z > b)
            def _():
                pl.when(z < line - 1)(lambda: add_arrived(k, base, b, b, extra))
                z_copy(k, base, b, b, {"dp": z - 1}, extra).start()

    def both_halves(pass_one):
        def body(k):
            pl.when(k % per_layer == 0)(lambda: pass_one(k, other, True))
            pass_one(k, own, False)
        return body

    def put(k, values):
        layer, q = place(k)
        out_ref[layer, :, pl.ds(pl.multiple_of(q * width, 128), width)] = values
        squares[layer] = squares[layer] + values * values

    def finish_one(k, base, extra):
        pl.when(z > 0)(lambda: add_arrived(k, base, z, z + 1, extra))
        pl.when(z < line - 1)(lambda: add_arrived(k, base, z, z, extra))
        if extra:
            late_copy(k // per_layer).start()
        else:
            pl.when(k % per_layer > 0)(lambda: put(k, block(k, base, z)[...]))

    def step(t, _):
        when_chunk(t, stage_partner)
        when_chunk(t - 1, merge_core)
        when_chunk(t - LAG, merge_y)
        back = line - 1 - z
        when_chunk(t - LAG - z, both_halves(to_right))
        when_chunk(t - LAG - back, both_halves(to_left))
        when_chunk(t - LAG - jnp.maximum(z, back), both_halves(finish_one))
        return 0

    lax.fori_loop(0, chunks + LAG + line - 1, step, 0)

    for layer in range(layers):
        late_copy(layer).wait_recv()
        put(layer * per_layer, block(layer * per_layer, own, z)[...] + late_y[layer])

    totals = cnt_ref[...]
    for d in range(1, experts):
        sender = lax.rem(e + d, experts)
        count_copy(d, sender).wait_recv()
        totals = totals + seen[sender]
    row = lax.broadcasted_iota(jnp.int32, totals.shape, 0)
    lane = lax.broadcasted_iota(jnp.int32, totals.shape, 1)
    for layer in range(layers):
        share = jnp.sum(jnp.sum(squares[layer], axis=0, keepdims=True), axis=1, keepdims=True)
        totals = jnp.where(row == layer, share, totals)
    message[...] = totals
    gathered[me] = totals

    def all_copy(d, sender):
        return remote(
            message, gathered.at[sender], all_send.at[d], all_recv.at[sender], group_peer(d)[1]
        )

    for d in range(1, group):
        all_copy(d, me).start()
    for d in range(1, group):
        all_copy(d, group_peer(d)[0]).wait_recv()
    total = gathered[0]
    for p in range(1, group):
        total = total + gathered[p]
    stats = jnp.zeros_like(total)
    for layer in range(layers):
        loads = total[layers + layer:layers + layer + 1, :]
        spot = lane[:1]
        own_load = jnp.sum(jnp.where(spot == e, loads, 0.0), axis=1, keepdims=True)
        mean_load = jnp.sum(jnp.where(spot < experts, loads, 0.0), axis=1, keepdims=True) / experts
        root_mean = jnp.sqrt(total[layer:layer + 1, :1] / numel)
        factor = (
            step_size * (own_load / mean_load) * clip_level / jnp.maximum(root_mean, clip_level)
        )
        beta = own_load / (own_load + mean_load)
        stats = jnp.where(row == layer, factor, stats)
        stats = jnp.where(row == layers + layer, beta, stats)
    stat_ref[...] = stats

    for d in range(1, group):
        all_copy(d, me).wait_send()
    for d in range(1, experts):
        count_copy(d, e).wait_send()
    for k in range(chunks - min(SLOTS, chunks), chunks):
        core_copy(k).wait_send()

    def drain(k, _):
        pl.when(k % per_layer > 0)(lambda: y_copy(k).wait_send())
        for b in range(line):
            pl.when(z != b)(lambda: z_copy(k, own, b, b, {"dp": z}, False).wait_send())
        return 0

    lax.fori_loop(0, chunks, drain, 0)
    for layer in range(layers):
        late_copy(layer).wait_send()
        for b in range(line):
            pl.when(z != b)(
                lambda: z_copy(layer * per_layer, other, b, b, {"dp": z}, True).wait_send()
            )


def on_device(sizes, activations, out_grads, weights, shadow, counts):
    line, experts, shards = sizes
    layers, _, tokens, all_rows = activations.shape
    ff, rows = out_grads.shape[3], weights.shape[2]
    assert shards == 2 * CORES and 2 * layers <= 8
    units = ff // 128
    per_layer = next(p for p in range(6, units + 1) if units % p == 0 and units // p % 2 == 0)
    width = ff // per_layer
    chunks = layers * per_layer
    half = line * rows
    group = line * shards
    acts = activations[:, 0].reshape(layers, tokens, line, shards // CORES, CORES, rows)
    acts = acts.transpose(0, 4, 3, 2, 5, 1).reshape(layers, CORES, all_rows // CORES, tokens)
    tile = jnp.pad(
        counts[:, 0, :].astype(jnp.float32), ((layers, 8 - 2 * layers), (0, 128 - experts))
    )
    f32 = jnp.float32
    dma = pltpu.SemaphoreType.DMA
    vmem = pl.BlockSpec(memory_space=pltpu.VMEM)
    dims = (line, experts, shards, layers, per_layer, width, rows, all_rows * ff)
    summed, stats = pl.pallas_call(
        functools.partial(kernel, dims),
        out_shape=(
            jax.ShapeDtypeStruct((layers, rows, ff), f32), jax.ShapeDtypeStruct((8, 128), f32)
        ),
        in_specs=[vmem] * 3,
        out_specs=(vmem, vmem),
        scratch_shapes=[
            pltpu.VMEM((chunks, 2 * half, width), f32),
            pltpu.VMEM((chunks, half, width), f32),
            pltpu.VMEM((chunks, line + 1, rows, width), f32),
            pltpu.VMEM((layers, line + 1, rows, width), f32),
            pltpu.VMEM((layers, rows, width), f32),
            pltpu.VMEM((SLOTS, 2 * half, width), f32),
            pltpu.VMEM((layers, rows, width), f32),
            pltpu.VMEM((experts, 8, 128), f32),
            pltpu.VMEM((8, 128), f32),
            pltpu.VMEM((group, 8, 128), f32),
            dma((SLOTS,)), dma((chunks,)), dma((chunks,)), dma((chunks,)),
            dma((chunks, line)), dma((chunks, line + 1)),
            dma((layers, line)), dma((layers, line + 1)),
            dma((layers,)), dma((layers,)), dma((experts,)), dma((experts,)),
            dma((group,)), dma((group,)),
        ],
        compiler_params=pltpu.CompilerParams(
            collective_id=0, has_side_effects=True, vmem_limit_bytes=62 * 1024 * 1024
        ),
        name="reduce_gradient",
    )(acts, out_grads[:, 0], tile)
    factor = stats[:layers, 0][:, None, None]
    beta = stats[layers:2 * layers, 0][:, None, None]
    updated = weights[:, 0] - factor * summed
    previous = shadow[:, 0]
    return updated[:, None], (previous + beta * (updated - previous))[:, None]


def solution(mesh):
    rows = P(None, "expert", ("dp", "shard"), None)
    in_specs = (rows, rows, rows, rows, P(None, ("dp", "expert", "shard"), None))
    sizes = tuple(mesh.shape[a] for a in ("dp", "expert", "shard"))
    return jax.shard_map(
        functools.partial(on_device, sizes), mesh=mesh, in_specs=in_specs,
        out_specs=(rows, rows), check_vma=False,
    )
```
